256 devices in a mesh: rep: 2 (over core), dp: 128 (over x, y, z).
Axes of the slice: x: 4, y: 4, z: 8, core: 2. Of those that a mesh axis runs over, the one named last changes fastest.
Arguments:
- x: bfloat16 [256, 2048, 512], P(('rep', 'dp')), parts along dimension 0
- dy: bfloat16 [256, 2048, 512], P(('rep', 'dp')), parts along dimension 0
- w_gate: bfloat16 [2, 512, 2048], replicated
- w_up: bfloat16 [2, 512, 2048], replicated
- w_down: bfloat16 [2, 2048, 512], replicated
- m_w_gate: float32 [2, 512, 2048], replicated
- m_w_up: float32 [2, 512, 2048], replicated
- m_w_down: float32 [2, 2048, 512], replicated
- v_w_gate: float32 [2, 512, 2048], replicated
- v_w_up: float32 [2, 512, 2048], replicated
- v_w_down: float32 [2, 2048, 512], replicated
Outputs:
- output 1: bfloat16 [4, 512, 2048], P('rep'), parts along dimension 0
- output 2: bfloat16 [4, 512, 2048], P('rep'), parts along dimension 0
- output 3: bfloat16 [4, 2048, 512], P('rep'), parts along dimension 0
- output 4: float32 [4, 512, 2048], P('rep'), parts along dimension 0
- output 5: float32 [4, 512, 2048], P('rep'), parts along dimension 0
- output 6: float32 [4, 2048, 512], P('rep'), parts along dimension 0
- output 7: float32 [4, 512, 2048], P('rep'), parts along dimension 0
- output 8: float32 [4, 512, 2048], P('rep'), parts along dimension 0
- output 9: float32 [4, 2048, 512], P('rep'), parts along dimension 0
There are 2 independent parts. The reference program is written for one: setup_inputs(seed, part) draws one part's arguments, and reference() takes and returns one part's arrays. A program takes and returns all parts, laid end to end along the dimension named above; an argument that names none is the same for every part.
All inputs are finite; a program needn't handle non-finite values.
Results may differ from the reference program's by a relative error of at most 0.022.
Values are sent between devices in bfloat16 or wider.
A program may use at most 768 MiB of HBM per device.

```python
import jax
import jax.numpy as jnp
from jax import lax

SEQUENCES = 128
TOKENS = 2048
D = 512
FF = 2048
LAYERS = 2
NAMES = ("w_gate", "w_up", "w_down")
SHAPES = {"w_gate": (LAYERS, D, FF), "w_up": (LAYERS, D, FF), "w_down": (LAYERS, FF, D)}


def bump(key, n, height):
    away = (jnp.arange(n, dtype=jnp.int32) - jax.random.randint(key, (), 0, n, jnp.int32)) % n
    return jnp.where(away < n // 8, height, 1.0)


def together(key, own, strength):
    shared = jax.random.normal(key, own.shape[1:], jnp.float32)
    return (own + strength * shared) * lax.rsqrt(1 + strength * strength)


def setup_inputs(seed: int = 0, part: int = 0) -> dict:
    kx, kdy, ka, kb, kz, kf, kh, kl, *keys = jax.random.split(jax.random.key(seed), 8 + 3 * len(NAMES))
    kx, kdy, ka, kb = (jax.random.fold_in(k, part) for k in (kx, kdy, ka, kb))
    kw, km, kv = (keys[i::3] for i in range(3))
    shape = (SEQUENCES, TOKENS, D)
    much_x, much_dy = jax.random.uniform(kz, (2,), jnp.float32, 0.0, 1.0)
    loud = 2.0 ** jax.random.uniform(jax.random.fold_in(kz, 1), (), jnp.float32, -1.0, 2.0)
    layers = 2.0 ** jax.random.uniform(kl, (LAYERS, 1, 1), jnp.float32, -1.0, 1.0)
    x = together(ka, jax.random.normal(kx, shape, jnp.float32), much_x) * bump(kf, D, 4.0)
    dy = together(kb, jax.random.normal(kdy, shape, jnp.float32), much_dy)
    drawn = {"x": x.astype(jnp.bfloat16), "dy": (loud * dy * (SEQUENCES * TOKENS) ** -0.5).astype(jnp.bfloat16)}
    for key, name in zip(kw, NAMES, strict=True):
        w = jax.random.normal(key, SHAPES[name], jnp.float32) * SHAPES[name][1] ** -0.5
        drawn[name] = (w * {"w_gate": 1.0, "w_up": bump(kh, FF, 4.0), "w_down": layers}[name]).astype(jnp.bfloat16)
    for key, name in zip(km, NAMES, strict=True):
        drawn[f"m_{name}"] = 0.1 * jax.random.normal(key, SHAPES[name], jnp.float32)
    for key, name in zip(kv, NAMES, strict=True):
        drawn[f"v_{name}"] = jax.random.uniform(key, SHAPES[name], jnp.float32, 0.005, 0.015)
    return drawn


def matmul(a, w):
    return jnp.dot(a, w, preferred_element_type=jnp.float32).astype(jnp.bfloat16)


def normed(h):
    wide = h.astype(jnp.float32)
    scale = lax.rsqrt(jnp.mean(wide**2, -1, keepdims=True) + 1e-6)
    return (wide * scale).astype(jnp.bfloat16)


def layer(h, w):
    a = normed(h)
    gate = jnp.dot(a, w["w_gate"], preferred_element_type=jnp.float32)
    up = jnp.dot(a, w["w_up"], preferred_element_type=jnp.float32)
    return h + matmul((jax.nn.silu(gate) * up).astype(jnp.bfloat16), w["w_down"])


def adamw(w, m, v, g):
    m = 0.9 * m + 0.1 * g
    v = 0.95 * v + 0.05 * g * g
    step = m * lax.rsqrt(v + 1e-8) + 0.1 * w
    return (w - 0.02 * step).astype(jnp.bfloat16), m, v


def clipped(gradients, sum_of_squares, count):
    factor = jnp.minimum(1.0, 0.5 * lax.rsqrt(sum_of_squares / count + 1e-30))
    return [g * factor for g in gradients]


def stack(weights, h):
    return lax.scan(lambda h, w: (layer(h, w), None), h, weights)[0]


def reference(x, dy, w_gate, w_up, w_down, m_w_gate, m_w_up, m_w_down, v_w_gate, v_w_up, v_w_down):
    weights = dict(zip(NAMES, (w_gate, w_up, w_down), strict=True))

    def take(so_far, sequence):
        h, by_y = sequence
        _, back = jax.vjp(lambda w: stack(w, h), weights)
        return jax.tree.map(lambda total, term: total + term.astype(jnp.float32), so_far, back(by_y)[0]), None

    none_yet = {name: jnp.zeros(w.shape, jnp.float32) for name, w in weights.items()}
    by_weights, _ = lax.scan(take, none_yet, (x, dy))
    gradients = [by_weights[name].astype(jnp.bfloat16).astype(jnp.float32) for name in NAMES]
    gradients = clipped(gradients, sum(jnp.sum(g * g) for g in gradients), sum(g.size for g in gradients))
    new = [
        adamw(w.astype(jnp.float32), m, v, g)
        for w, m, v, g in zip((w_gate, w_up, w_down), (m_w_gate, m_w_up, m_w_down), (v_w_gate, v_w_up, v_w_down), gradients, strict=True)
    ]
    return tuple(one[which] for which in range(3) for one in new)
```

```python
import functools
import heapq

import jax
import jax.numpy as jnp
from jax import lax
from jax.experimental import pallas as pl
from jax.experimental.pallas import tpu as pltpu
from jax.sharding import PartitionSpec as P

NAMES = ("w_gate", "w_up", "w_down")
SIZES = {"x": 4, "y": 4, "z": 8}
LANES = 512
MESH = pl.DeviceIdType.MESH
ORDERS = (("x", "y", "z"), ("y", "z", "x"), ("z", "x", "y"))


def matmul(a, w):
    return jnp.dot(a, w, preferred_element_type=jnp.float32).astype(jnp.bfloat16)


def normed(h):
    wide = h.astype(jnp.float32)
    scale = lax.rsqrt(jnp.mean(wide**2, -1, keepdims=True) + 1e-6)
    return (wide * scale).astype(jnp.bfloat16)


def layer(h, w):
    a = normed(h)
    gate = jnp.dot(a, w["w_gate"], preferred_element_type=jnp.float32)
    up = jnp.dot(a, w["w_up"], preferred_element_type=jnp.float32)
    return h + matmul((jax.nn.silu(gate) * up).astype(jnp.bfloat16), w["w_down"])


def position():
    dp = lax.axis_index("dp")
    ny, nz = SIZES["y"], SIZES["z"]
    return {"x": dp // (ny * nz), "y": (dp // nz) % ny, "z": dp % nz}


def along(me, axis, delta):
    at = dict(me)
    at[axis] = (me[axis] + delta + SIZES[axis]) % SIZES[axis]
    return {"dp": (at["x"] * SIZES["y"] + at["y"]) * SIZES["z"] + at["z"]}


def meet(me):
    barrier = pltpu.get_barrier_semaphore()
    count = 0
    for axis, n in SIZES.items():
        for delta in range(1, n):
            pl.semaphore_signal(barrier, inc=1, device_id=along(me, axis, delta), device_id_type=MESH)
            count += 1
    pl.semaphore_wait(barrier, count)


def cut(axes, axis, i, wide):
    lead = (slice(None),) * axes.index(axis)
    if wide and axis == "z":
        return lead + (i // 4, slice(None), pl.ds(pl.multiple_of((i % 4) * LANES, LANES), LANES))
    return lead + (i,)


def shape_of(axes, wide):
    if wide and "z" in axes:
        return tuple(SIZES[a] for a in axes if a != "z") + (SIZES["z"] // 4, 16, 4 * LANES)
    return tuple(SIZES[a] for a in axes) + (16, LANES)


def at(index, lead):
    out, rest = [], list(lead)
    for part in index:
        out.append(rest.pop(0) if isinstance(part, slice) and rest else part)
    return tuple(out[: len(index)]) + tuple(rest)


def add_into(slot, local, index):
    shape = slot.shape[:-2]
    total = 1
    for n in shape:
        total *= n

    def body(i, _):
        lead, rest = [], i
        for n in reversed(shape):
            lead.insert(0, rest % n)
            rest = rest // n
        term = local[at(index, lead)].astype(jnp.float32)
        slot[tuple(lead)] = (slot[tuple(lead)].astype(jnp.float32) + term).astype(slot.dtype)
        return 0

    lax.fori_loop(0, total, body, 0, unroll=False)


def reduce_one(me, number, wide, order, sign, grad, slots, sends, recvs, out, drain):
    axes, local, copy_number, near = ("x", "y", "z"), grad, 0, 1.0
    for phase in range(2):
        axis = order[phase]
        n, p, buffer = SIZES[axis], me[axis], slots[phase]
        near /= n
        target = along(me, axis, sign)
        for t in range(n - 1):
            source = local.at[cut(axes, axis, (p - sign + n) % n, wide)] if t == 0 else buffer.at[t - 1]
            copy = pltpu.make_async_remote_copy(
                src_ref=source,
                dst_ref=buffer.at[t],
                send_sem=sends.at[copy_number],
                recv_sem=recvs.at[copy_number],
                device_id=target,
                device_id_type=MESH,
            )
            copy.start()
            drain.append(copy)
            copy_number += 1
            yield 2.2 + 45.0 * near
            copy.wait_recv()
            add_into(buffer.at[t], local, cut(axes, axis, (p - sign * (t + 2) + 2 * n) % n, wide))
        local = buffer.at[n - 2]
        axes = tuple(a for a in axes if a != axis)
    axis = order[2]
    n, p, buffer = SIZES[axis], me[axis], slots[2]
    copies = []
    for delta in range(1, n):
        copy = pltpu.make_async_remote_copy(
            src_ref=local.at[cut(axes, axis, (p + delta) % n, wide)],
            dst_ref=buffer.at[delta - 1],
            send_sem=sends.at[copy_number],
            recv_sem=recvs.at[copy_number],
            device_id=along(me, axis, delta),
            device_id_type=MESH,
        )
        copy.start()
        drain.append(copy)
        copies.append(copy)
        copy_number += 1
    yield 1.0 + 0.9 * n
    total = local[cut(axes, axis, p, wide)].astype(jnp.float32)
    for delta in range(1, n):
        copies[delta - 1].wait_recv()
        total = total + buffer[delta - 1].astype(jnp.float32)
    out[...] = total.astype(out.dtype)


def scatter_kernel(*refs):
    grads, outs, rest = refs[:6], refs[6:9], refs[9:]
    me = position()
    meet(me)
    drain, waiting = [], []
    for number in range(6):
        which, layer_number = number % 3, number // 3
        slots, sends, recvs = rest[5 * number : 5 * number + 3], rest[5 * number + 3], rest[5 * number + 4]
        one = reduce_one(
            me, number, which < 2, ORDERS[which], 1 - 2 * layer_number, grads[number], slots, sends, recvs, outs[which].at[layer_number], drain
        )
        waiting.append((next(one), number, one))
    heapq.heapify(waiting)
    while waiting:
        now, number, one = heapq.heappop(waiting)
        step = next(one, None)
        if step is not None:
            heapq.heappush(waiting, (now + step, number, one))
    for copy in drain:
        copy.wait_send()


def reduce_scatter(grads):
    scratch = []
    for number in range(6):
        which = number % 3
        axes, count = ("x", "y", "z"), 0
        for phase in range(3):
            n = SIZES[ORDERS[which][phase]]
            axes = tuple(a for a in axes if a != ORDERS[which][phase])
            scratch.append(pltpu.VMEM((n - 1,) + shape_of(axes, which < 2), jnp.bfloat16))
            count += n - 1
        scratch += [pltpu.SemaphoreType.DMA((count,))] * 2
    return pl.pallas_call(
        scatter_kernel,
        out_shape=[jax.ShapeDtypeStruct((2, 16, LANES), jnp.bfloat16)] * 3,
        in_specs=[pl.BlockSpec(memory_space=pltpu.VMEM)] * 6,
        out_specs=[pl.BlockSpec(memory_space=pltpu.VMEM)] * 3,
        scratch_shapes=scratch,
        compiler_params=pltpu.CompilerParams(collective_id=0, has_side_effects=True, vmem_limit_bytes=40 << 20),
        name="reduce_scatter",
    )(*grads)


def norm_kernel(count, a_ref, b_ref, c_ref, factor_ref, *rest):
    slots, sends, recvs = rest[:3], rest[3], rest[4]
    me = position()
    meet(me)
    total = jnp.zeros((8, 128), jnp.float32)
    for ref in (a_ref, b_ref, c_ref):
        for number in range(2):
            wide = ref[number].astype(jnp.float32)
            wide = wide * wide
            for rows in range(0, 16, 8):
                for columns in range(0, LANES, 128):
                    total = total + wide[rows : rows + 8, columns : columns + 128]
    copy_number, drain = 0, []
    for (axis, n), buffer in zip(SIZES.items(), slots, strict=True):
        p = me[axis]
        buffer[p] = total
        copies = []
        for delta in range(1, n):
            copy = pltpu.make_async_remote_copy(
                src_ref=buffer.at[p],
                dst_ref=buffer.at[p],
                send_sem=sends.at[copy_number],
                recv_sem=recvs.at[copy_number],
                device_id=along(me, axis, delta),
                device_id_type=MESH,
            )
            copy.start()
            copies.append(copy)
            copy_number += 1
        for copy in copies:
            copy.wait_recv()
        total = buffer[0]
        for i in range(1, n):
            total = total + buffer[i]
        drain += copies
    mean = jnp.sum(total, keepdims=True) / count
    factor_ref[...] = jnp.broadcast_to(jnp.minimum(1.0, 0.5 * lax.rsqrt(mean + 1e-30)), factor_ref.shape)
    for copy in drain:
        copy.wait_send()


def clip_factor(shares, count):
    copies = sum(n - 1 for n in SIZES.values())
    return pl.pallas_call(
        functools.partial(norm_kernel, count),
        out_shape=jax.ShapeDtypeStruct((8, 128), jnp.float32),
        in_specs=[pl.BlockSpec(memory_space=pltpu.VMEM)] * 3,
        out_specs=pl.BlockSpec(memory_space=pltpu.VMEM),
        scratch_shapes=[pltpu.VMEM((n, 8, 128), jnp.float32) for n in SIZES.values()] + [pltpu.SemaphoreType.DMA((copies,))] * 2,
        compiler_params=pltpu.CompilerParams(collective_id=1, has_side_effects=True, vmem_limit_bytes=4 << 20),
        cost_estimate=pl.CostEstimate(flops=20_000_000, bytes_accessed=200_000, transcendentals=0),
        name="clip_factor",
    )(*shares)


def adamw_kernel(wide, factor_ref, g_ref, w_ref, m_ref, v_ref, w_out, m_out, v_out):
    factor = factor_ref[0:1, 0:1]
    rows = w_ref.shape[1]
    across = 4 if wide else 1

    def body(r, _):
        here = pl.ds(pl.multiple_of(r * 16, 16), 16)
        for k in range(across):
            columns = pl.ds(k * LANES, LANES)
            g = g_ref[0, r * across + k].astype(jnp.float32) * factor
            m = 0.9 * m_ref[0, here, columns] + 0.1 * g
            v = 0.95 * v_ref[0, here, columns] + 0.05 * g * g
            w = w_ref[0, here, columns].astype(jnp.float32)
            step = m * lax.rsqrt(v + 1e-8) + 0.1 * w
            w_out[0, here, columns] = (w - 0.02 * step).astype(jnp.bfloat16)
            m_out[0, here, columns] = m
            v_out[0, here, columns] = v
        return 0

    lax.fori_loop(0, rows // 16, body, 0, unroll=2)


def adamw(w, m, v, g, factor):
    layers, rows, columns = w.shape
    wide = columns > LANES
    block = min(rows, 262144 // columns)
    tiles = block // 16 * (columns // LANES)
    whole = pl.BlockSpec((1, block, columns), lambda i, j: (i, j, 0))
    size = w.size
    return pl.pallas_call(
        functools.partial(adamw_kernel, wide),
        grid=(layers, rows // block),
        out_shape=[jax.ShapeDtypeStruct(w.shape, t) for t in (jnp.bfloat16, jnp.float32, jnp.float32)],
        in_specs=[pl.BlockSpec((8, 128), lambda i, j: (0, 0)), pl.BlockSpec((1, tiles, 16, LANES), lambda i, j: (i, j, 0, 0)), whole, whole, whole],
        out_specs=[whole] * 3,
        compiler_params=pltpu.CompilerParams(vmem_limit_bytes=63 << 20),
        cost_estimate=pl.CostEstimate(flops=16 * size, bytes_accessed=22 * size, transcendentals=size),
        name="adamw",
    )(factor, g, w, m, v)


def optimizer(grads, weights, m, v):
    count = sum(w.size for w in weights)
    x, y, z = SIZES.values()
    cutup = [g.reshape((x, y, z, 16, LANES) if i % 3 == 2 else (x, y, z // 4, 16, 4 * LANES)) for i, g in enumerate(grads)]
    shares = reduce_scatter(cutup)
    gathered = [lax.all_gather(s, "dp", axis=1, tiled=True).reshape(2, -1, 16, LANES) for s in shares]
    factor = clip_factor(shares, count)
    new = [adamw(w, m, v, g, factor) for w, m, v, g in zip(weights, m, v, gathered, strict=True)]
    return tuple(one[which] for which in range(3) for one in new)


def solution(mesh):
    def step(x, dy, *arrays):
        weights, m, v = (arrays[i : i + 3] for i in (0, 3, 6))
        layers = weights[0].shape[0]
        h, kept = x[0], []
        for number in range(layers):
            kept.append(h)
            h = layer(h, {name: w[number] for name, w in zip(NAMES, weights, strict=True)})
        by_h, grads = dy[0], [None] * layers
        for number in reversed(range(layers)):
            _, back = jax.vjp(lambda w, h: layer(h, w), {name: w[number] for name, w in zip(NAMES, weights, strict=True)}, kept[number])
            by_w, by_h = back(by_h)
            grads[number] = [by_w[name] for name in NAMES]
        return optimizer(grads[0] + grads[1], weights, m, v)

    return jax.shard_map(
        step,
        mesh=mesh,
        in_specs=(P(("rep", "dp"), None, None),) * 2 + (P(None, None, None),) * 9,
        out_specs=(P("rep", None, None),) * 9,
        check_vma=False,
    )
```

```python
import functools
import heapq

import jax
import jax.numpy as jnp
from jax import lax
from jax.experimental import pallas as pl
from jax.experimental.pallas import tpu as pltpu
from jax.sharding import PartitionSpec as P

NAMES = ("w_gate", "w_up", "w_down")
SIZES = {"x": 4, "y": 4, "z": 8}
LANES = 512
MESH = pl.DeviceIdType.MESH
ORDERS = (("x", "y", "z"), ("y", "z", "x"), ("z", "x", "y"))


TOKENS = 512
HIDDEN = 256


def dot(a, b, on=(1, 0)):
    return lax.dot_general(a, b, (((on[0],), (on[1],)), ((), ())), preferred_element_type=jnp.float32)


def gradients_kernel(x_ref, dy_ref, wg_ref, wu_ref, wd_ref, *refs):
    (gg0, gu0, gd0, gg1, gu1, gd1), (a_ref, h_ref, b_ref, hid_ref, dgate_ref, dup_ref, one_ref, two_ref) = refs[:6], refs[6:]
    tokens, d = x_ref.shape
    ff = wg_ref.shape[2]

    def over(n, size, body):
        def at_step(i, _):
            body(pl.ds(pl.multiple_of(i * size, size), size))
            return 0

        lax.fori_loop(0, n // size, at_step, 0)

    def norm(source, target):
        def rows(t):
            wide = source[t, :].astype(jnp.float32)
            target[t, :] = (wide * lax.rsqrt(jnp.mean(wide * wide, -1, keepdims=True) + 1e-6)).astype(jnp.bfloat16)

        over(tokens, 128, rows)

    def zero(ref):
        def rows(t):
            ref[t, :] = jnp.zeros((128, d), jnp.float32)

        over(tokens, 128, rows)

    norm(x_ref, a_ref)
    zero(one_ref)

    def forward(f):
        def rows(t):
            a = a_ref[t, :]
            gate, up = dot(a, wg_ref[0, :, f]), dot(a, wu_ref[0, :, f])
            hidden = (gate * jax.nn.sigmoid(gate) * up).astype(jnp.bfloat16)
            one_ref[t, :] += dot(hidden, wd_ref[0, f, :])

        over(tokens, TOKENS, rows)

    over(ff, HIDDEN, forward)

    def add(t):
        h = x_ref[t, :].astype(jnp.float32) + one_ref[t, :].astype(jnp.bfloat16).astype(jnp.float32)
        h_ref[t, :] = h.astype(jnp.bfloat16)

    over(tokens, 128, add)

    def backward(number, a_ref, by_ref, gg, gu, gd, more):
        def hidden_block(f):
            def rows(t):
                a, by = a_ref[t, :], by_ref[t, :]
                gate, up = dot(a, wg_ref[number, :, f]), dot(a, wu_ref[number, :, f])
                by_hidden = dot(by, wd_ref[number, f, :], (1, 1)).astype(jnp.bfloat16).astype(jnp.float32)
                sigmoid = jax.nn.sigmoid(gate)
                silu = gate * sigmoid
                hid_ref[t, :] = (silu * up).astype(jnp.bfloat16)
                dup = (by_hidden * silu).astype(jnp.bfloat16)
                dgate = (by_hidden * up * (sigmoid + silu * (1.0 - sigmoid))).astype(jnp.bfloat16)
                dgate_ref[t, :] = dgate
                dup_ref[t, :] = dup
                if more:
                    one_ref[t, :] += dot(dgate, wg_ref[number, :, f], (1, 1))
                    two_ref[t, :] += dot(dup, wu_ref[number, :, f], (1, 1))

            over(tokens, TOKENS, rows)
            gd[f, :] = dot(hid_ref[...], by_ref[...], (0, 0)).astype(jnp.bfloat16)
            gg[:, f] = dot(a_ref[...], dgate_ref[...], (0, 0)).astype(jnp.bfloat16)
            gu[:, f] = dot(a_ref[...], dup_ref[...], (0, 0)).astype(jnp.bfloat16)

        over(ff, HIDDEN, hidden_block)

    norm(h_ref, b_ref)
    zero(one_ref)
    zero(two_ref)
    backward(1, b_ref, dy_ref, gg1, gu1, gd1, True)

    def by_norm(t):
        wide = h_ref[t, :].astype(jnp.float32)
        by = (one_ref[t, :].astype(jnp.bfloat16).astype(jnp.float32) + two_ref[t, :].astype(jnp.bfloat16).astype(jnp.float32))
        by = by.astype(jnp.bfloat16).astype(jnp.float32)
        scale = lax.rsqrt(jnp.mean(wide * wide, -1, keepdims=True) + 1e-6)
        inner = jnp.mean(by * wide, -1, keepdims=True)
        by_h = (by * scale - wide * (inner * scale * scale * scale)).astype(jnp.bfloat16).astype(jnp.float32)
        b_ref[t, :] = (dy_ref[t, :].astype(jnp.float32) + by_h).astype(jnp.bfloat16)

    over(tokens, 128, by_norm)
    backward(0, a_ref, b_ref, gg0, gu0, gd0, False)


def gradients(x, dy, w_gate, w_up, w_down):
    tokens, d = x.shape
    ff = w_gate.shape[2]
    shapes = [(d, ff), (d, ff), (ff, d)] * 2
    flops = 17 * 2 * tokens * d * ff
    return pl.pallas_call(
        gradients_kernel,
        out_shape=[jax.ShapeDtypeStruct(s, jnp.bfloat16) for s in shapes],
        in_specs=[pl.BlockSpec(memory_space=pltpu.VMEM)] * 5,
        out_specs=[pl.BlockSpec(memory_space=pltpu.VMEM)] * 6,
        scratch_shapes=[pltpu.VMEM((tokens, d), jnp.bfloat16)] * 3
        + [pltpu.VMEM((tokens, HIDDEN), jnp.bfloat16)] * 3
        + [pltpu.VMEM((tokens, d), jnp.float32)] * 2,
        compiler_params=pltpu.CompilerParams(vmem_limit_bytes=63 << 20),
        cost_estimate=pl.CostEstimate(flops=flops, bytes_accessed=30 << 20, transcendentals=3 * tokens * ff),
        name="gradients",
    )(x, dy, w_gate, w_up, w_down)


def position():
    dp = lax.axis_index("dp")
    ny, nz = SIZES["y"], SIZES["z"]
    return {"x": dp // (ny * nz), "y": (dp // nz) % ny, "z": dp % nz}


def along(me, axis, delta):
    at = dict(me)
    at[axis] = (me[axis] + delta + SIZES[axis]) % SIZES[axis]
    return {"dp": (at["x"] * SIZES["y"] + at["y"]) * SIZES["z"] + at["z"]}


def meet(me):
    barrier = pltpu.get_barrier_semaphore()
    count = 0
    for axis, n in SIZES.items():
        for delta in range(1, n):
            pl.semaphore_signal(barrier, inc=1, device_id=along(me, axis, delta), device_id_type=MESH)
            count += 1
    pl.semaphore_wait(barrier, count)


def cut(axes, axis, i, wide):
    lead = (slice(None),) * axes.index(axis)
    if wide and axis == "z":
        return lead + (i // 4, slice(None), pl.ds(pl.multiple_of((i % 4) * LANES, LANES), LANES))
    return lead + (i,)


def shape_of(axes, wide):
    if wide and "z" in axes:
        return tuple(SIZES[a] for a in axes if a != "z") + (SIZES["z"] // 4, 16, 4 * LANES)
    return tuple(SIZES[a] for a in axes) + (16, LANES)


def at(index, lead):
    out, rest = [], list(lead)
    for part in index:
        out.append(rest.pop(0) if isinstance(part, slice) and rest else part)
    return tuple(out[: len(index)]) + tuple(rest)


def add_into(slot, local, index):
    shape = slot.shape[:-2]
    total = 1
    for n in shape:
        total *= n

    def body(i, _):
        lead, rest = [], i
        for n in reversed(shape):
            lead.insert(0, rest % n)
            rest = rest // n
        term = local[at(index, lead)].astype(jnp.float32)
        slot[tuple(lead)] = (slot[tuple(lead)].astype(jnp.float32) + term).astype(slot.dtype)
        return 0

    lax.fori_loop(0, total, body, 0, unroll=False)


def region(fixed, wide):
    lead = tuple(fixed.get(axis, slice(None)) for axis in "xy")
    if "z" not in fixed:
        return lead
    if wide:
        return lead + (fixed["z"] // 4, slice(None), pl.ds(pl.multiple_of((fixed["z"] % 4) * LANES, LANES), LANES))
    return lead + (fixed["z"],)


def sum_one(me, wide, order, sign, grad, slots, sends, recvs, out, squares, drain):
    axes, local, near = ("x", "y", "z"), grad, 1.0
    numbers = iter(range(1000))

    def send(source, target, to):
        number = next(numbers)
        copy = pltpu.make_async_remote_copy(
            src_ref=source, dst_ref=target, send_sem=sends.at[number], recv_sem=recvs.at[number], device_id=to, device_id_type=MESH
        )
        copy.start()
        drain.append(copy)
        return copy

    for phase in range(2):
        axis = order[phase]
        n, p, buffer = SIZES[axis], me[axis], slots[phase]
        near /= n
        target = along(me, axis, sign)
        for t in range(n - 1):
            source = local.at[cut(axes, axis, (p - sign + n) % n, wide)] if t == 0 else buffer.at[t - 1]
            copy = send(source, buffer.at[t], target)
            yield 2.2 + 46.0 * near
            copy.wait_recv()
            add_into(buffer.at[t], local, cut(axes, axis, (p - sign * (t + 2) + 2 * n) % n, wide))
        local = buffer.at[n - 2]
        axes = tuple(a for a in axes if a != axis)
    axis = order[2]
    n, p, buffer = SIZES[axis], me[axis], slots[2]
    copies = [
        send(local.at[cut(axes, axis, (p + delta) % n, wide)], buffer.at[delta - 1], along(me, axis, delta)) for delta in range(1, n)
    ]
    yield 1.0 + 0.9 * n
    total = local[cut(axes, axis, p, wide)].astype(jnp.float32)
    for delta in range(1, n):
        copies[delta - 1].wait_recv()
        total = total + buffer[delta - 1].astype(jnp.float32)
    total = total.astype(out.dtype)
    mine = region(me, wide)
    out[mine] = total
    wide_total = total.astype(jnp.float32)
    wide_total = wide_total * wide_total
    square = jnp.zeros((8, 128), jnp.float32)
    for rows in range(0, 16, 8):
        for columns in range(0, LANES, 128):
            square = square + wide_total[rows : rows + 8, columns : columns + 128]
    squares[...] = square
    copies = [send(out.at[mine], out.at[mine], along(me, axis, delta)) for delta in range(1, n)]
    yield "reduced"
    yield 1.0 + 0.9 * n
    for copy in copies:
        copy.wait_recv()
    fixed = dict(me)
    for phase in (1, 0):
        fixed.pop(order[phase + 1])
        axis = order[phase]
        n, p = SIZES[axis], me[axis]
        target = along(me, axis, sign)
        for t in range(n - 1):
            block = out.at[region({**fixed, axis: (p - sign * t + n) % n}, wide)]
            copy = send(block, block, target)
            yield 2.2 + 46.0 * near
            copy.wait_recv()
        near *= n


def norm_one(me, count, squares, factor, slots, sends, recvs, drain):
    total = squares[0]
    for number in range(1, 6):
        total = total + squares[number]
    copy_number = 0
    for (axis, n), buffer in zip(SIZES.items(), slots, strict=True):
        p = me[axis]
        buffer[p] = total
        copies = []
        for delta in range(1, n):
            copy = pltpu.make_async_remote_copy(
                src_ref=buffer.at[p],
                dst_ref=buffer.at[p],
                send_sem=sends.at[copy_number],
                recv_sem=recvs.at[copy_number],
                device_id=along(me, axis, delta),
                device_id_type=MESH,
            )
            copy.start()
            copies.append(copy)
            copy_number += 1
        yield 1.0 + 0.9 * n
        for copy in copies:
            copy.wait_recv()
        total = buffer[0]
        for i in range(1, n):
            total = total + buffer[i]
        drain += copies
    mean = jnp.sum(total, keepdims=True) / count
    factor[...] = jnp.broadcast_to(jnp.minimum(1.0, 0.5 * lax.rsqrt(mean + 1e-30)), factor.shape)


def sum_kernel(count, *refs):
    grads, outs, factor, squares, norm, rest = refs[:6], refs[6:9], refs[9], refs[10], refs[11:16], refs[16:]
    me = position()
    meet(me)
    drain, waiting, reduced = [], [], 0
    for number in range(6):
        which, layer_number = number % 3, number // 3
        slots, sends, recvs = rest[5 * number : 5 * number + 3], rest[5 * number + 3], rest[5 * number + 4]
        sign = 1 - 2 * layer_number
        out = outs[which].at[layer_number]
        one = sum_one(me, which < 2, ORDERS[which], sign, grads[number], slots, sends, recvs, out, squares.at[number], drain)
        waiting.append((next(one), number, one))
    heapq.heapify(waiting)
    while waiting:
        now, number, one = heapq.heappop(waiting)
        step = next(one, None)
        if step == "reduced":
            reduced += 1
            if reduced == 6:
                last = norm_one(me, count, squares, factor, norm[:3], norm[3], norm[4], drain)
                heapq.heappush(waiting, (now + next(last), 6, last))
            step = next(one)
        if step is not None:
            heapq.heappush(waiting, (now + step, number, one))
    for copy in drain:
        copy.wait_send()


def sums(grads, count):
    scratch = [pltpu.VMEM((6, 8, 128), jnp.float32)] + [pltpu.VMEM((n, 8, 128), jnp.float32) for n in SIZES.values()]
    steps = sum(n - 1 for n in SIZES.values())
    scratch += [pltpu.SemaphoreType.DMA((steps,))] * 2
    for number in range(6):
        which = number % 3
        axes = ("x", "y", "z")
        for phase in range(3):
            axes = tuple(a for a in axes if a != ORDERS[which][phase])
            scratch.append(pltpu.VMEM((SIZES[ORDERS[which][phase]] - 1,) + shape_of(axes, which < 2), jnp.bfloat16))
        scratch += [pltpu.SemaphoreType.DMA((2 * steps,))] * 2
    return pl.pallas_call(
        functools.partial(sum_kernel, count),
        out_shape=[jax.ShapeDtypeStruct((2,) + shape_of(("x", "y", "z"), i < 2), jnp.bfloat16) for i in range(3)]
        + [jax.ShapeDtypeStruct((8, 128), jnp.float32)],
        in_specs=[pl.BlockSpec(memory_space=pltpu.VMEM)] * 6,
        out_specs=[pl.BlockSpec(memory_space=pltpu.VMEM)] * 4,
        scratch_shapes=scratch,
        compiler_params=pltpu.CompilerParams(collective_id=0, has_side_effects=True, vmem_limit_bytes=44 << 20),
        cost_estimate=pl.CostEstimate(flops=100_000_000_000, bytes_accessed=24 << 20, transcendentals=0),
        name="sums",
    )(*grads)


def adamw_kernel(factor_ref, *refs):
    factor = factor_ref[0:1, 0:1]
    for k in range(3):
        (g_ref, w_ref, m_ref, v_ref), (w_out, m_out, v_out) = refs[4 * k : 4 * k + 4], refs[12 + 3 * k : 15 + 3 * k]
        rows, columns = w_ref.shape[1:]

        def body(r, _):
            here = (0, pl.ds(pl.multiple_of(r * 16, 16), 16))
            for c in range(0, columns, LANES):
                at = here + (pl.ds(c, LANES),)
                g = g_ref[at].astype(jnp.float32) * factor
                m = 0.9 * m_ref[at] + 0.1 * g
                v = 0.95 * v_ref[at] + 0.05 * g * g
                w = w_ref[at].astype(jnp.float32)
                step = m * lax.rsqrt(v + 1e-8) + 0.1 * w
                w_out[at] = (w - 0.02 * step).astype(jnp.bfloat16)
                m_out[at] = m
                v_out[at] = v
            return 0

        lax.fori_loop(0, rows // 16, body, 0, unroll=max(1, LANES * 4 // columns))


def adamw(weights, m, v, g, factor, steps=8):
    blocks = [pl.BlockSpec((1, w.shape[1] // steps, w.shape[2]), lambda i, j: (i, j, 0)) for w in weights]
    size = sum(w.size for w in weights)
    shapes = [jax.ShapeDtypeStruct(w.shape, t) for w in weights for t in (jnp.bfloat16, jnp.float32, jnp.float32)]
    out = pl.pallas_call(
        adamw_kernel,
        grid=(weights[0].shape[0], steps),
        out_shape=shapes,
        in_specs=[pl.BlockSpec((8, 128), lambda i, j: (0, 0))] + [block for block in blocks for _ in range(4)],
        out_specs=[block for block in blocks for _ in range(3)],
        compiler_params=pltpu.CompilerParams(vmem_limit_bytes=63 << 20),
        cost_estimate=pl.CostEstimate(flops=16 * size, bytes_accessed=22 * size, transcendentals=size),
        name="adamw",
    )(factor, *(one for four in zip(g, weights, m, v, strict=True) for one in four))
    return [out[3 * k : 3 * k + 3] for k in range(3)]


def optimizer(grads, weights, m, v):
    count = sum(w.size for w in weights)
    cutup = [g.reshape(shape_of(("x", "y", "z"), i % 3 < 2)) for i, g in enumerate(grads)]
    *summed, factor = sums(cutup, count)
    new = adamw(weights, m, v, [s.reshape(w.shape) for s, w in zip(summed, weights, strict=True)], factor)
    return tuple(one[which] for which in range(3) for one in new)


def solution(mesh):
    def step(x, dy, *arrays):
        weights, m, v = (arrays[i : i + 3] for i in (0, 3, 6))
        return optimizer(gradients(x[0], dy[0], *weights), weights, m, v)

    return jax.shard_map(
        step,
        mesh=mesh,
        in_specs=(P(("rep", "dp"), None, None),) * 2 + (P(None, None, None),) * 9,
        out_specs=(P("rep", None, None),) * 9,
        check_vma=False,
    )
```

```python
import functools
import heapq

import jax
import jax.numpy as jnp
from jax import lax
from jax.experimental import pallas as pl
from jax.experimental.pallas import tpu as pltpu
from jax.sharding import PartitionSpec as P

NAMES = ("w_gate", "w_up", "w_down")
SIZES = {"x": 4, "y": 4, "z": 8}
LANES = 256
TOKENS = 512
HIDDEN = 256
MESH = pl.DeviceIdType.MESH
ORDERS = (("x", "y", "z"), ("y", "z", "x"), ("z", "x", "y"))


def dot(a, b, on=(1, 0)):
    return lax.dot_general(a, b, (((on[0],), (on[1],)), ((), ())), preferred_element_type=jnp.float32)


def position():
    dp = lax.axis_index("dp")
    ny, nz = SIZES["y"], SIZES["z"]
    return {"x": dp // (ny * nz), "y": (dp // nz) % ny, "z": dp % nz}


def along(me, axis, delta):
    at = dict(me)
    at[axis] = (me[axis] + delta + SIZES[axis]) % SIZES[axis]
    return {"dp": (at["x"] * SIZES["y"] + at["y"]) * SIZES["z"] + at["z"]}


def columns_at(base, z=None):
    return pl.ds(base, LANES) if z is None else pl.ds(pl.multiple_of(base + (z % 4) * LANES, LANES), LANES)


def region(fixed, wide, base):
    lead = tuple(fixed.get(axis, slice(None)) for axis in "xy")
    if "z" in fixed:
        return lead + ((fixed["z"] // 4, slice(None), columns_at(base, fixed["z"])) if wide else (fixed["z"], slice(None), columns_at(base)))
    return lead + (slice(None), slice(None), pl.ds(base, 4 * LANES if wide else LANES))


def cut(axes, axis, i, wide):
    lead = (slice(None),) * axes.index(axis)
    if wide and axis == "z":
        return lead + (i // 4, slice(None), columns_at(0, i))
    return lead + (i,)


def shape_of(axes, wide, halves=1):
    if wide and "z" in axes:
        return tuple(SIZES[a] for a in axes if a != "z") + (SIZES["z"] // 4, 16, 4 * halves * LANES)
    return tuple(SIZES[a] for a in axes) + (16, halves * LANES)


def at(index, lead, dims):
    full, rest = list(index) + [slice(None)] * (dims - len(index)), iter(lead)
    return tuple(next(rest) if k < dims - 2 and isinstance(part, slice) else part for k, part in enumerate(full))


def add_into(slot, local, index):
    shape, dims = slot.shape[:-2], len(local.shape)
    total = 1
    for n in shape:
        total *= n

    def body(i, _):
        lead, rest = [], i
        for n in reversed(shape):
            lead.insert(0, rest % n)
            rest = rest // n
        term = local[at(index, lead, dims)].astype(jnp.float32)
        slot[tuple(lead)] = (slot[tuple(lead)].astype(jnp.float32) + term).astype(slot.dtype)
        return 0

    lax.fori_loop(0, total, body, 0)


def sum_one(me, wide, base, order, sign, grad, slots, sends, recvs, out, squares, drain):
    axes, local, near = ("x", "y", "z"), None, 1.0
    numbers = iter(range(1000))

    def send(source, target, to):
        number = next(numbers)
        copy = pltpu.make_async_remote_copy(
            src_ref=source, dst_ref=target, send_sem=sends.at[number], recv_sem=recvs.at[number], device_id=to, device_id_type=MESH
        )
        copy.start()
        drain.append(copy)
        return copy

    for phase in range(2):
        axis = order[phase]
        n, p, buffer = SIZES[axis], me[axis], slots[phase]
        near /= n
        target = along(me, axis, sign)

        def block(i):
            return region({axis: i % n}, wide, base) if local is None else cut(axes, axis, i % n, wide)

        held = grad if local is None else local
        for t in range(n - 1):
            source = held.at[block(p - sign + n)] if t == 0 else buffer.at[t - 1]
            copy = send(source, buffer.at[t], target)
            yield 2.2 + 23.0 * near
            copy.wait_recv()
            add_into(buffer.at[t], held, block(p - sign * (t + 2) + 2 * n))
        local = buffer.at[n - 2]
        axes = tuple(a for a in axes if a != axis)
    axis = order[2]
    n, p, buffer = SIZES[axis], me[axis], slots[2]
    copies = [
        send(local.at[cut(axes, axis, (p + delta) % n, wide)], buffer.at[delta - 1], along(me, axis, delta)) for delta in range(1, n)
    ]
    yield 1.0 + 0.7 * n
    total = local[cut(axes, axis, p, wide)].astype(jnp.float32)
    for delta in range(1, n):
        copies[delta - 1].wait_recv()
        total = total + buffer[delta - 1].astype(jnp.float32)
    total = total.astype(out.dtype)
    mine = region(me, wide, base)
    out[mine] = total
    wide_total = total.astype(jnp.float32)
    wide_total = wide_total * wide_total
    width = squares.shape[-1]
    square = jnp.zeros((8, width), jnp.float32)
    for rows in range(0, 16, 8):
        for columns in range(0, LANES, width):
            square = square + wide_total[rows : rows + 8, columns : columns + width]
    squares[...] = square
    copies = [send(out.at[mine], out.at[mine], along(me, axis, delta)) for delta in range(1, n)]
    yield "reduced"
    yield 1.0 + 0.7 * n
    for copy in copies:
        copy.wait_recv()
    fixed = dict(me)
    for phase in (1, 0):
        fixed.pop(order[phase + 1])
        axis = order[phase]
        n, p = SIZES[axis], me[axis]
        target = along(me, axis, sign)
        for t in range(n - 1):
            part = out.at[region({**fixed, axis: (p - sign * t + n) % n}, wide, base)]
            copy = send(part, part, target)
            yield 2.2 + 23.0 * near
            copy.wait_recv()
        near *= n


def norm_one(me, count, squares, factor, slots, sends, recvs, drain):
    total = squares[0]
    for number in range(1, squares.shape[0]):
        total = total + squares[number]
    copy_number = 0
    for (axis, n), buffer in zip(SIZES.items(), slots, strict=True):
        p = me[axis]
        buffer[p] = total
        copies = []
        for delta in range(1, n):
            copy = pltpu.make_async_remote_copy(
                src_ref=buffer.at[p],
                dst_ref=buffer.at[p],
                send_sem=sends.at[copy_number],
                recv_sem=recvs.at[copy_number],
                device_id=along(me, axis, delta),
                device_id_type=MESH,
            )
            copy.start()
            copies.append(copy)
            copy_number += 1
        yield 1.0 + 0.7 * n
        for copy in copies:
            copy.wait_recv()
        total = buffer[0]
        for i in range(1, n):
            total = total + buffer[i]
        drain += copies
    mean = jnp.sum(total, keepdims=True) / count
    factor[...] = jnp.broadcast_to(jnp.minimum(1.0, 0.5 * lax.rsqrt(mean + 1e-30)), factor.shape)


class Flows:
    def __init__(self, last):
        self.now, self.waiting, self.reduced, self.made, self.last = 0.0, [], 0, 0, last

    def add(self, one):
        heapq.heappush(self.waiting, (self.now + next(one), self.made, one))
        self.made += 1

    def until(self, time):
        while self.waiting and self.waiting[0][0] <= time:
            due, number, one = heapq.heappop(self.waiting)
            self.now = max(self.now, due)
            step = next(one, None)
            if step == "reduced":
                self.reduced += 1
                if self.reduced == 12:
                    self.add(self.last())
                step = next(one)
            if step is not None:
                heapq.heappush(self.waiting, (self.now + step, number, one))
        self.now = max(self.now, time)


def step_kernel(count, x_ref, dy_ref, wg_hbm, wu_hbm, wd_hbm, *refs):
    outs, factor, rest = refs[:3], refs[3], refs[4:]
    a_ref, h_ref, b_ref, hid_ref, dgate_ref, dup_ref, one_ref, two_ref, wg_ref, wu_ref, wd_ref, w_sems, x_sem = rest[:13]
    grads, squares, norm, flow_refs = (rest[13:16], rest[16:19]), rest[19], rest[20:25], rest[25:]
    tokens, d = x_ref.shape
    ff = wg_hbm.shape[2]
    blocks = ff // HIDDEN
    me = position()

    barrier = pltpu.get_barrier_semaphore()
    peers = [(axis, delta) for axis, n in SIZES.items() for delta in range(1, n)]
    for axis, delta in peers:
        pl.semaphore_signal(barrier, inc=1, device_id=along(me, axis, delta), device_id_type=MESH)

    def fetch(number, i, slot):
        f = pl.ds(pl.multiple_of(i * HIDDEN, HIDDEN), HIDDEN)
        return (
            pltpu.make_async_copy(wg_hbm.at[number, :, f], wg_ref.at[slot], w_sems.at[slot, 0]),
            pltpu.make_async_copy(wu_hbm.at[number, :, f], wu_ref.at[slot], w_sems.at[slot, 1]),
            pltpu.make_async_copy(wd_hbm.at[number, f, :], wd_ref.at[slot], w_sems.at[slot, 2]),
        )

    def turn(number, i, after):
        if after is not None:
            later = i + 1
            for copy in fetch(number + (later // blocks) * (after - number), later % blocks, later % 2):
                copy.start()
        for copy in fetch(number, i, i % 2):
            copy.wait()

    def over(n, size, body):
        def at_step(i, _):
            body(pl.ds(pl.multiple_of(i * size, size), size))
            return 0

        lax.fori_loop(0, n // size, at_step, 0)

    def normed(source, target):
        def rows(t):
            wide = source[t, :].astype(jnp.float32)
            target[t, :] = (wide * lax.rsqrt(jnp.mean(wide * wide, -1, keepdims=True) + 1e-6)).astype(jnp.bfloat16)

        over(tokens, min(128, tokens), rows)

    def zero(ref):
        def rows(t):
            ref[t, :] = jnp.zeros((min(128, tokens), d), jnp.float32)

        over(tokens, min(128, tokens), rows)

    take = pltpu.make_async_copy(x_ref, h_ref, x_sem)
    take.start()
    for copy in fetch(0, 0, 0):
        copy.start()
    take.wait()

    normed(h_ref, a_ref)
    zero(one_ref)

    def forward(i, _):
        turn(0, i, 1)
        slot = i % 2

        def rows(t):
            a = a_ref[t, :]
            gate, up = dot(a, wg_ref[slot]), dot(a, wu_ref[slot])
            hidden = (gate * jax.nn.sigmoid(gate) * up).astype(jnp.bfloat16)
            one_ref[t, :] += dot(hidden, wd_ref[slot])

        over(tokens, TOKENS, rows)
        return 0

    lax.fori_loop(0, blocks, forward, 0)

    def add(t):
        h = h_ref[t, :].astype(jnp.float32) + one_ref[t, :].astype(jnp.bfloat16).astype(jnp.float32)
        h_ref[t, :] = h.astype(jnp.bfloat16)

    over(tokens, min(128, tokens), add)

    def backward(number, i, after, more, a_ref, by_ref):
        turn(number, i, after)
        slot = i % 2
        gg, gu, gd = grads[number]

        def rows(t):
            a, by = a_ref[t, :], by_ref[t, :]
            gate, up = dot(a, wg_ref[slot]), dot(a, wu_ref[slot])
            by_hidden = dot(by, wd_ref[slot], (1, 1)).astype(jnp.bfloat16).astype(jnp.float32)
            sigmoid = jax.nn.sigmoid(gate)
            silu = gate * sigmoid
            hid_ref[t, :] = (silu * up).astype(jnp.bfloat16)
            dup = (by_hidden * silu).astype(jnp.bfloat16)
            dgate = (by_hidden * up * (sigmoid + silu * (1.0 - sigmoid))).astype(jnp.bfloat16)
            dgate_ref[t, :] = dgate
            dup_ref[t, :] = dup
            if more:
                one_ref[t, :] += dot(dgate, wg_ref[slot], (1, 1))
                two_ref[t, :] += dot(dup, wu_ref[slot], (1, 1))

        over(tokens, TOKENS, rows)
        x, y, z = SIZES.values()
        f = pl.ds(i * HIDDEN, HIDDEN) if isinstance(i, int) else pl.ds(pl.multiple_of(i * HIDDEN, HIDDEN), HIDDEN)
        pairs = HIDDEN // (16 * z)
        first = i * pairs
        down = dot(hid_ref[...], by_ref[...], (0, 0)).astype(jnp.bfloat16)
        gd[first // y, pl.ds(first % y, pairs)] = down.reshape(pairs, z, 16, d)
        for ref, by_ff in ((gg, dgate_ref), (gu, dup_ref)):
            across = dot(a_ref[...], by_ff[...], (0, 0)).astype(jnp.bfloat16)
            ref[:, :, :, :, f] = across.reshape(x, y, z // 4, 16, HIDDEN)

    normed(h_ref, b_ref)
    zero(one_ref)
    zero(two_ref)

    def last_layer(i, _):
        backward(1, i, 0, True, b_ref, dy_ref)
        return 0

    lax.fori_loop(0, blocks, last_layer, 0)

    drain = []
    flows = Flows(lambda: norm_one(me, count, squares, factor, norm[:3], norm[3], norm[4], drain))

    def start(number):
        for half in range(2):
            for which in range(3):
                place = (number * 2 + half) * 3 + which
                slots, sends, recvs = flow_refs[5 * place : 5 * place + 3], flow_refs[5 * place + 3], flow_refs[5 * place + 4]
                base = half * (4 * LANES if which < 2 else LANES)
                out = outs[which].at[number]
                flows.add(
                    sum_one(
                        me, which < 2, base, ORDERS[which], 1 - 2 * half, grads[number][which], slots, sends, recvs, out, squares.at[place], drain
                    )
                )

    pl.semaphore_wait(barrier, len(peers))
    start(1)

    def by_norm(t):
        wide = h_ref[t, :].astype(jnp.float32)
        by = one_ref[t, :].astype(jnp.bfloat16).astype(jnp.float32) + two_ref[t, :].astype(jnp.bfloat16).astype(jnp.float32)
        by = by.astype(jnp.bfloat16).astype(jnp.float32)
        scale = lax.rsqrt(jnp.mean(wide * wide, -1, keepdims=True) + 1e-6)
        inner = jnp.mean(by * wide, -1, keepdims=True)
        by_h = (by * scale - wide * (inner * scale * scale * scale)).astype(jnp.bfloat16).astype(jnp.float32)
        b_ref[t, :] = (dy_ref[t, :].astype(jnp.float32) + by_h).astype(jnp.bfloat16)

    over(tokens, min(128, tokens), by_norm)
    flows.until(2.0)
    for i in range(blocks):
        backward(0, i, 0 if i + 1 < blocks else None, False, a_ref, b_ref)
        flows.until(2.0 + 3.4 * (i + 1))
    start(0)
    flows.until(1e9)
    for copy in drain:
        copy.wait_send()


def sums(x, dy, w_gate, w_up, w_down):
    tokens, d = x.shape
    layers, _, ff = w_gate.shape
    width = min(128, LANES)
    shapes = [shape_of(("x", "y", "z"), i < 2, 2) for i in range(3)]
    steps = sum(n - 1 for n in SIZES.values())
    scratch = [pltpu.VMEM((tokens, d), jnp.bfloat16)] * 3 + [pltpu.VMEM((tokens, HIDDEN), jnp.bfloat16)] * 3
    scratch += [pltpu.VMEM((tokens, d), jnp.float32)] * 2
    scratch += [pltpu.VMEM((2, d, HIDDEN), jnp.bfloat16)] * 2 + [pltpu.VMEM((2, HIDDEN, d), jnp.bfloat16)]
    scratch += [pltpu.SemaphoreType.DMA((2, 3)), pltpu.SemaphoreType.DMA]
    scratch += [pltpu.VMEM(shape, jnp.bfloat16) for shape in shapes * 2]
    scratch += [pltpu.VMEM((12, 8, width), jnp.float32)] + [pltpu.VMEM((n, 8, width), jnp.float32) for n in SIZES.values()]
    scratch += [pltpu.SemaphoreType.DMA((steps,))] * 2
    for place in range(12):
        which = place % 3
        axes = ("x", "y", "z")
        for phase in range(3):
            axes = tuple(a for a in axes if a != ORDERS[which][phase])
            scratch.append(pltpu.VMEM((SIZES[ORDERS[which][phase]] - 1,) + shape_of(axes, which < 2), jnp.bfloat16))
        scratch += [pltpu.SemaphoreType.DMA((2 * steps,))] * 2
    return pl.pallas_call(
        functools.partial(step_kernel, layers * 3 * d * ff),
        out_shape=[jax.ShapeDtypeStruct((layers,) + shape, jnp.bfloat16) for shape in shapes] + [jax.ShapeDtypeStruct((8, 128), jnp.float32)],
        in_specs=[pl.BlockSpec(memory_space=pl.ANY), pl.BlockSpec(memory_space=pltpu.VMEM)] + [pl.BlockSpec(memory_space=pl.ANY)] * 3,
        out_specs=[pl.BlockSpec(memory_space=pltpu.VMEM)] * 4,
        scratch_shapes=scratch,
        compiler_params=pltpu.CompilerParams(collective_id=0, has_side_effects=True, vmem_limit_bytes=67043328),
        cost_estimate=pl.CostEstimate(flops=34 * tokens * d * ff, bytes_accessed=60 << 20, transcendentals=3 * tokens * ff),
        name="sums",
    )(x, dy, w_gate, w_up, w_down)


def adamw_kernel(factor_ref, *refs):
    factor = factor_ref[0:1, 0:1]
    for k in range(3):
        (g_ref, w_ref, m_ref, v_ref), (w_out, m_out, v_out) = refs[4 * k : 4 * k + 4], refs[12 + 3 * k : 15 + 3 * k]
        rows, columns = w_ref.shape[1:]

        def body(r, _):
            here = (0, pl.ds(pl.multiple_of(r * 16, 16), 16))
            for c in range(0, columns, 512):
                at = here + (pl.ds(c, 512),)
                g = g_ref[at].astype(jnp.float32) * factor
                m = 0.9 * m_ref[at] + 0.1 * g
                v = 0.95 * v_ref[at] + 0.05 * g * g
                w = w_ref[at].astype(jnp.float32)
                step = m * lax.rsqrt(v + 1e-8) + 0.1 * w
                w_out[at] = (w - 0.02 * step).astype(jnp.bfloat16)
                m_out[at] = m
                v_out[at] = v
            return 0

        lax.fori_loop(0, rows // 16, body, 0, unroll=max(1, 512 * 4 // columns))


def adamw(weights, m, v, g, factor, steps=8):
    blocks = [pl.BlockSpec((1, w.shape[1] // steps, w.shape[2]), lambda i, j: (i, j, 0)) for w in weights]
    size = sum(w.size for w in weights)
    shapes = [jax.ShapeDtypeStruct(w.shape, t) for w in weights for t in (jnp.bfloat16, jnp.float32, jnp.float32)]
    out = pl.pallas_call(
        adamw_kernel,
        grid=(weights[0].shape[0], steps),
        out_shape=shapes,
        in_specs=[pl.BlockSpec((8, 128), lambda i, j: (0, 0))] + [block for block in blocks for _ in range(4)],
        out_specs=[block for block in blocks for _ in range(3)],
        compiler_params=pltpu.CompilerParams(vmem_limit_bytes=63 << 20),
        cost_estimate=pl.CostEstimate(flops=16 * size, bytes_accessed=22 * size, transcendentals=size),
        name="adamw",
    )(factor, *(one for four in zip(g, weights, m, v, strict=True) for one in four))
    return [out[3 * k : 3 * k + 3] for k in range(3)]


def solution(mesh):
    def step(x, dy, *arrays):
        weights, m, v = (arrays[i : i + 3] for i in (0, 3, 6))
        *summed, factor = sums(x[0], dy[0], *weights)
        new = adamw(weights, m, v, [s.reshape(w.shape) for s, w in zip(summed, weights, strict=True)], factor)
        return tuple(one[which] for which in range(3) for one in new)

    return jax.shard_map(
        step,
        mesh=mesh,
        in_specs=(P(("rep", "dp"), None, None),) * 2 + (P(None, None, None),) * 9,
        out_specs=(P("rep", None, None),) * 9,
        check_vma=False,
    )
```
